1024 devices in a mesh: gx: 8 (over z_lo), gy: 4 (over z_hi, core), ta: 32 (over x, y).
Axes of the slice: x: 4, y: 8, z: 16 (z_hi: 2, z_lo: 8; z = z_hi * 8 + z_lo), core: 2. Of those that a mesh axis runs over, the one named last changes fastest.
Arguments:
- links: float32 [4, 2, 3, 3, 16, 8, 32, 128], P(None, None, None, None, 'gx', 'gy', 'ta'), may hold values from -1 to 1, as said below
Outputs:
- flowed: float32 [4, 2, 3, 3, 16, 8, 32, 128], P(None, None, None, None, 'gx', 'gy', 'ta')
- action_slices: float32 [32], P('ta')
The draws below stay inside these ranges and needn't reach their ends.
Inputs may be any that keep to these rules, and one draw needn't show every extreme that they name: `links`: every link is a special unitary 3x3 matrix.
All inputs are finite; a program needn't handle non-finite values.
Results may differ from the reference program's by a relative error of at most 0.0003.
Values sent between devices are 32-bit elements; how exact they have to be, the bound alone decides.
No kernel may reach another device: no remote copies, remote signals or barrier semaphores. Data moves between devices by JAX's collectives and lax.ppermute only.
A program may use at most 32 MiB of HBM per device.

```python
import jax
import jax.numpy as jnp
from jax import lax

NZ = 128
NX = 16
NY = 8
NT = 32


def complex_times(former, latter):
    return jnp.stack([former[0] * latter[0] - former[1] * latter[1], former[0] * latter[1] + former[1] * latter[0]])


def normalized(vector):
    length = jnp.sqrt(jnp.sum(vector[0] ** 2 + vector[1] ** 2, axis=0))
    return vector / length


def draw_links(key, part):
    raw = jax.random.normal(key, (2, 3, 3, 4, NX, NY, NT, NZ), jnp.float32)
    row_zero = normalized(raw[:, 0])
    second = raw[:, 1]
    inner_real = jnp.sum(row_zero[0] * second[0] + row_zero[1] * second[1], axis=0)
    inner_imag = jnp.sum(row_zero[0] * second[1] - row_zero[1] * second[0], axis=0)
    projection = jnp.stack([inner_real * row_zero[0] - inner_imag * row_zero[1], inner_real * row_zero[1] + inner_imag * row_zero[0]])
    row_one = normalized(second - projection)
    pieces = []
    for first_col, second_col in ((1, 2), (2, 0), (0, 1)):
        cross = complex_times(row_zero[:, first_col], row_one[:, second_col]) - complex_times(row_zero[:, second_col], row_one[:, first_col])
        pieces.append(jnp.stack([cross[0], -cross[1]]))
    row_two = jnp.stack(pieces, axis=1)
    matrix = jnp.stack([row_zero, row_one, row_two], axis=1)
    return jnp.moveaxis(matrix, 3, 0)


def setup_inputs(seed: int = 0) -> dict:
    key_list = jax.random.split(jax.random.key(seed), 2)
    links = draw_links(jax.random.fold_in(key_list[1], 71), 0)
    return {"links": links}


flow_eps = 0.1
taylor_order = 6


def contract(first_part, second_part):
    return jnp.sum(first_part[:, :, None] * second_part[None, :, :], axis=1)


def matmul_pair(former, latter):
    return jnp.stack([contract(former[0], latter[0]) - contract(former[1], latter[1]),
                      contract(former[0], latter[1]) + contract(former[1], latter[0])])


def adjoint(matrix):
    return jnp.stack([jnp.swapaxes(matrix[0], 0, 1), -jnp.swapaxes(matrix[1], 0, 1)])


def trace_real(former, latter):
    return jnp.sum(former[0] * jnp.swapaxes(latter[0], 0, 1) - former[1] * jnp.swapaxes(latter[1], 0, 1), axis=(0, 1))


def unit_offset(dir_index, sign):
    return tuple(sign if k == dir_index else 0 for k in range(4))


def add_offsets(first_off, second_off):
    return tuple(first_off[k] + second_off[k] for k in range(4))


def shifted(component, offset):
    x_len = component.shape[-4] - 2
    y_len = component.shape[-3] - 2
    t_len = component.shape[-2] - 2
    view = component[..., 1 + offset[0]:1 + offset[0] + x_len, 1 + offset[1]:1 + offset[1] + y_len,
                     1 + offset[2]:1 + offset[2] + t_len, :]
    if offset[3] != 0:
        view = jnp.roll(view, -offset[3], axis=-1)
    return view


def upper_staple(padded, mu_dir, nu_dir):
    here = (0, 0, 0, 0)
    first_pair = matmul_pair(shifted(padded[nu_dir], unit_offset(mu_dir, 1)),
                             adjoint(shifted(padded[mu_dir], unit_offset(nu_dir, 1))))
    return matmul_pair(first_pair, adjoint(shifted(padded[nu_dir], here)))


def lower_corner(padded, mu_dir, nu_dir):
    back = unit_offset(nu_dir, -1)
    corner = add_offsets(unit_offset(mu_dir, 1), back)
    first_pair = matmul_pair(adjoint(shifted(padded[nu_dir], corner)), adjoint(shifted(padded[mu_dir], back)))
    return matmul_pair(first_pair, shifted(padded[nu_dir], back))


def antihermitian(matrix):
    real_part = (matrix[0] - jnp.swapaxes(matrix[0], 0, 1)) / 2.0
    imag_part = (matrix[1] + jnp.swapaxes(matrix[1], 0, 1)) / 2.0
    trace_imag = jnp.trace(matrix[1], axis1=0, axis2=1) / 3.0
    eye = jnp.eye(3, dtype=jnp.float32).reshape((3, 3) + (1,) * (matrix.ndim - 3))
    return jnp.stack([real_part, imag_part - eye * trace_imag])


def flow_force(padded, lower_fn):
    centre = padded[..., 1:-1, 1:-1, 1:-1, :]
    forces = []
    action = jnp.zeros((centre.shape[6],), jnp.float32)
    for mu_dir in range(4):
        link_here = centre[mu_dir]
        staple_sum = jnp.zeros_like(link_here)
        for nu_dir in range(4):
            if nu_dir == mu_dir:
                continue
            upper = upper_staple(padded, mu_dir, nu_dir)
            action = action + jnp.sum(1.0 - trace_real(link_here, upper) / 3.0, axis=(0, 1, 3))
            staple_sum = staple_sum + upper + lower_fn(mu_dir, nu_dir)
        omega = matmul_pair(link_here, staple_sum)
        forces.append(-flow_eps * antihermitian(omega))
    return jnp.stack(forces), action / 2.0


def polynomial_exp(generator):
    eye = jnp.eye(3, dtype=jnp.float32).reshape((3, 3) + (1,) * (generator.ndim - 3))
    identity = jnp.stack([jnp.broadcast_to(eye, generator.shape[1:]), jnp.zeros(generator.shape[1:], jnp.float32)])
    result = identity
    for order in range(taylor_order, 0, -1):
        result = identity + matmul_pair(generator, result) / order
    return result


def advance(generator, links_now):
    def one_direction(gen_dir, link_dir):
        return matmul_pair(polynomial_exp(gen_dir), link_dir)
    return jax.vmap(one_direction)(generator, links_now)


def section_force(links_now):
    extended = jnp.concatenate([links_now[..., -1:, :], links_now, links_now[..., :1, :]], axis=6)

    def slice_force(t_index):
        block = lax.dynamic_slice_in_dim(extended, t_index, 3, axis=6)
        padded = jnp.concatenate([block[..., -1:, :, :, :], block, block[..., :1, :, :, :]], axis=4)
        padded = jnp.concatenate([padded[..., -1:, :, :], padded, padded[..., :1, :, :]], axis=5)

        def lower_fn(mu_dir, nu_dir):
            return lower_corner(padded, mu_dir, nu_dir)
        return flow_force(padded, lower_fn)

    forces, action = lax.map(slice_force, jnp.arange(NT, dtype=jnp.int32))
    forces = jnp.moveaxis(forces[..., 0, :], 0, 6)
    return forces, action.reshape((NT,))


def reference(links):
    force_zero, action = section_force(links)
    section_one = advance(force_zero / 4.0, links)
    force_one, unused_one = section_force(section_one)
    section_two = advance(8.0 / 9.0 * force_one - 17.0 / 36.0 * force_zero, section_one)
    force_two, unused_two = section_force(section_two)
    flowed = advance(3.0 / 4.0 * force_two - 8.0 / 9.0 * force_one + 17.0 / 36.0 * force_zero, section_two)
    action_slices = action / (6.0 * NX * NY * NZ)
    return flowed, action_slices
```

```python
import functools

import jax
import jax.numpy as jnp
from jax import lax
from jax.experimental import pallas as pl
from jax.experimental.pallas import tpu as pltpu
from jax.sharding import PartitionSpec as P


INTERPRET = False

flow_eps = 0.1
X, Y, T, Z = 0, 1, 2, 3
NZ = 128


TWO_ROWS = (0, 1, 2, 3, 4, 5, 9, 10, 11, 12, 13, 14)
TWO_ROWS_CUTS = ((0, 6, 0), (9, 15, 6))
GENERATOR_CUTS = ((1, 3, 0), (5, 6, 2), (10, 12, 3), (14, 15, 5), (9, 10, 6), (13, 14, 7))


def message_form(stage):
    return (12, TWO_ROWS_CUTS, TWO_ROWS) if stage == 0 else (8, GENERATOR_CUTS, tuple(range(18)))


def message_shape(stage):
    faces, _, corners = message_form(stage)
    return (faces + len(corners) // 2, 8, NZ)


def comps(ref, *lead):
    return [ref[(*lead, c)] for c in range(18)]


def times(a, b, b_adjoint=False, a_adjoint=False):
    def ga(i, k):
        return (a[k * 3 + i], a[9 + k * 3 + i]) if a_adjoint else (a[i * 3 + k], a[9 + i * 3 + k])

    def gb(k, j):
        return (b[j * 3 + k], b[9 + j * 3 + k]) if b_adjoint else (b[k * 3 + j], b[9 + k * 3 + j])

    real, imag = [], []
    same = a_adjoint == b_adjoint
    for i in range(3):
        for j in range(3):
            rr = ii = ri = ir = None
            for k in range(3):
                ar, ai = ga(i, k)
                br, bi = gb(k, j)
                rr = ar * br if rr is None else rr + ar * br
                ii = ai * bi if ii is None else ii + ai * bi
                ri = ar * bi if ri is None else ri + ar * bi
                ir = ai * br if ir is None else ir + ai * br
            real.append(rr - ii if same else rr + ii)
            if a_adjoint:
                imag.append(ri - ir if not b_adjoint else -(ri + ir))
            else:
                imag.append(ri + ir if not b_adjoint else ir - ri)
    return real + imag


def put(ref, values, *lead):
    for c in range(18):
        ref[(*lead, c)] = values[c]


def roll_rows(v, shift):
    return pltpu.roll(v, shift, 0)


def roll_lanes(v, shift):
    return pltpu.roll(v, shift % NZ, 1)


def expo_times(x, w):
    x2 = times(x, x)
    x3 = times(x2, x)
    q = [x[c] * (1.0 / 24.0) + x2[c] * (1.0 / 120.0) + x3[c] * (1.0 / 720.0) for c in range(18)]
    r = times(x3, q)
    for c in range(18):
        r[c] = r[c] + (x[c] + x2[c] * 0.5 + x3[c] * (1.0 / 6.0))
    for c in (0, 4, 8):
        r[c] = r[c] + 1.0
    return times(r, w)


def third_row(ref, rows):
    for k, (i, j) in enumerate(((1, 2), (2, 0), (0, 1))):
        ari, aii, arj, aij = ref[i, rows], ref[9 + i, rows], ref[j, rows], ref[9 + j, rows]
        bri, bii, brj, bij = ref[3 + i, rows], ref[12 + i, rows], ref[3 + j, rows], ref[12 + j, rows]
        ref[6 + k, rows] = (ari * brj - aii * bij) - (arj * bri - aij * bii)
        ref[15 + k, rows] = (arj * bii + aij * bri) - (ari * bij + aii * brj)


def unpack_faces(stage, raw_ref, before_ref, full_ref):
    for h in range(raw_ref.shape[1] // 8):
        rows = slice(h * 8, h * 8 + 8)
        if stage == 0:
            for lo, hi, at in TWO_ROWS_CUTS:
                full_ref[lo:hi, rows] = raw_ref[at : at + hi - lo, rows]
            third_row(full_ref, rows)
            continue
        g = [raw_ref[m, rows] for m in range(8)]
        if stage == 1:
            g = [v * 0.25 for v in g]
        r01, r02, r12, i01, i02, i12, d0, d1 = g
        zero = jnp.zeros((8, NZ), jnp.float32)
        x = [zero, r01, r02, -r01, zero, r12, -r02, -r12, zero, d0, i01, i02, i01, d1, i12, i02, i12, -(d0 + d1)]
        new = expo_times(x, [before_ref[c, rows] for c in range(18)])
        for c in range(18):
            full_ref[c, rows] = new[c]


def unpack_corners(stage, raw_ref, full_ref):
    faces, _, corners = message_form(stage)
    for m, c in enumerate(corners):
        row = (m % 2) * 3
        full_ref[c, 8:11] = raw_ref[faces + m // 2, row : row + 3]
    if stage == 0:
        third_row(full_ref, slice(8, 16))


def row_ids(rows):
    return lax.broadcasted_iota(jnp.int32, (rows, NZ), 0)


def lane_ids(rows):
    return lax.broadcasted_iota(jnp.int32, (rows, NZ), 1)


def is_even(where_ref, k):
    return where_ref[k] % 2 == 0


def sort_pair(even, a_ref, b_ref, plus_ref, minus_ref):
    mask = jnp.broadcast_to(even, a_ref.shape[1:])
    for c in range(plus_ref.shape[0]):
        a, b = a_ref[c], b_ref[c]
        plus_ref[c] = jnp.where(mask, a, b)
        minus_ref[c] = jnp.where(mask, b, a)


def stage_kernel(stage, where_ref, s_ref, xp_ref, xm_ref, tp_ref, tm_ref, ya_ref, yb_ref, qa_ref, qb_ref, *rest):
    rest = list(rest)
    z_ref = rest.pop(0) if stage else None
    before = (rest.pop(0), rest.pop(0)) if stage else (None, None)
    act_ref = rest.pop(0) if stage == 1 else None
    s_out = rest.pop(0)
    if stage < 2:
        xa_out, xb_out, hop_out = rest.pop(0), rest.pop(0), rest.pop(0)
        z_out = rest.pop(0)
        act_out = rest.pop(0)
        plus_out, minus_out = rest.pop(0), rest.pop(0)
    v_ref, r_ref, t_ref, b_ref, u_ref, w_ref, g_ref = rest[:7]
    yp_ref, ym_ref, qp_ref, qm_ref, yp_raw, ym_raw, yp_face, ym_face = rest[7:]
    sort_pair(is_even(where_ref, 1), ya_ref, yb_ref, yp_raw, ym_raw)
    sort_pair(is_even(where_ref, 2), qa_ref, qb_ref, qp_ref, qm_ref)
    for k, (raw, face, full) in enumerate(((yp_raw, yp_face, yp_ref), (ym_raw, ym_face, ym_ref))):
        unpack_faces(stage, raw, before[k], face)
        full[:, 0:8] = face[...]
        unpack_corners(stage, raw, full)
    if stage < 2:
        plus_out[...] = yp_face[...]
        minus_out[...] = ym_face[...]

    own = lambda d: slice(d * 4, d * 4 + 4)
    for nu in range(4):
        for mu in range(4):
            v_ref[nu, mu, :, 0:4] = s_ref[:, own(mu)]
            if nu == X:
                v_ref[nu, mu, :, 6:8] = xm_ref[:, mu * 2 : mu * 2 + 2]
            elif nu == Y:
                v_ref[nu, mu, :, 7:8] = ym_ref[0:18, mu * 2 : mu * 2 + 1]
                v_ref[nu, mu, :, 5:6] = ym_ref[0:18, mu * 2 + 1 : mu * 2 + 2]
            elif nu == T:
                v_ref[nu, mu, :, 4:8] = tm_ref[:, own(mu)]
    for nu in range(4):
        if nu != X:
            r_ref[nu, X, :, 0:2] = s_ref[:, nu * 4 + 2 : nu * 4 + 4]
            r_ref[nu, X, :, 2:4] = xp_ref[:, nu * 2 : nu * 2 + 2]
        if nu != Y:
            r_ref[nu, Y, :, 0:1] = s_ref[:, nu * 4 + 1 : nu * 4 + 2]
            r_ref[nu, Y, :, 1:2] = yp_ref[0:18, nu * 2 : nu * 2 + 1]
            r_ref[nu, Y, :, 2:3] = s_ref[:, nu * 4 + 3 : nu * 4 + 4]
            r_ref[nu, Y, :, 3:4] = yp_ref[0:18, nu * 2 + 1 : nu * 2 + 2]
        if nu != T:
            r_ref[nu, T, :, 0:4] = tp_ref[:, own(nu)]
        if nu != Z:
            for c in range(18):
                r_ref[nu, Z, c] = roll_lanes(v_ref[nu, nu, c], -1)
    r_ref[X, Y, :, 6:7] = xm_ref[:, 1:2]
    r_ref[X, Y, :, 7:8] = yp_ref[0:18, 8:9]
    r_ref[X, T, :, 6:8] = qp_ref[...]
    r_ref[Y, X, :, 7:8] = ym_ref[0:18, 3:4]
    r_ref[Y, X, :, 5:6] = ym_ref[0:18, 8:9]
    r_ref[Y, T, :, 7:8] = ym_ref[0:18, 9:10]
    r_ref[Y, T, :, 5:6] = ym_ref[0:18, 10:11]
    r_ref[T, X, :, 4:6] = tm_ref[:, 10:12]
    r_ref[T, X, :, 6:8] = qm_ref[...]
    r_ref[T, Y, :, 4:5] = tm_ref[:, 9:10]
    r_ref[T, Y, :, 5:6] = yp_ref[0:18, 9:10]
    r_ref[T, Y, :, 6:7] = tm_ref[:, 11:12]
    r_ref[T, Y, :, 7:8] = yp_ref[0:18, 10:11]

    for mu in range(4):
        for c in range(18):
            b_ref[mu, c] = jnp.zeros((8, NZ), jnp.float32)
            u_ref[mu, c] = jnp.zeros((8, NZ), jnp.float32)
    rows = row_ids(8)
    for nu in range(4):

        def lower(m, carry, nu=nu):
            mu = m + (m >= nu).astype(jnp.int32)
            t = times(comps(v_ref, nu, mu), comps(r_ref, nu, mu))
            put(t_ref, t, nu, mu)
            low = times(t, comps(v_ref, nu, nu), a_adjoint=True)
            for c in range(18):
                v = low[c]
                if nu == X:
                    v = roll_rows(v, 2)
                elif nu == Y:
                    v = jnp.where(rows == 2, roll_rows(v, 5), roll_rows(v, 1))
                elif nu == T:
                    v = roll_rows(v, 4)
                else:
                    v = roll_lanes(v, 1)
                b_ref[mu, c] = b_ref[mu, c] + v
            return carry

        lax.fori_loop(0, 3, lower, 0)

    trace = None
    for mu in range(4):
        for nu in range(mu + 1, 4):
            p = times(comps(t_ref, nu, mu), comps(t_ref, mu, nu), b_adjoint=True)
            for i in range(3):
                for j in range(3):
                    k, l = i * 3 + j, j * 3 + i
                    u_ref[mu, k] = u_ref[mu, k] + p[k]
                    u_ref[mu, 9 + k] = u_ref[mu, 9 + k] + p[9 + k]
                    u_ref[nu, k] = u_ref[nu, k] + p[l]
                    u_ref[nu, 9 + k] = u_ref[nu, 9 + k] - p[9 + l]
            if stage == 0:
                part = 1.0 - (p[0] + p[4] + p[8]) / 3.0
                trace = part if trace is None else trace + part

    def force(mu, carry):
        omega = times(comps(v_ref, 3, mu), comps(b_ref, mu))
        omega = [omega[c] + u_ref[mu, c] for c in range(18)]
        mean = (omega[9] + omega[13] + omega[17]) / 3.0
        for i in range(3):
            for j in range(3):
                k, l = i * 3 + j, j * 3 + i
                g_ref[mu, k] = (-0.5 * flow_eps) * (omega[k] - omega[l])
                imag = 0.5 * (omega[9 + k] + omega[9 + l])
                if i == j:
                    imag = imag - mean
                g_ref[mu, 9 + k] = -flow_eps * imag
        return carry

    lax.fori_loop(0, 4, force, 0)
    for mu in range(4):
        w_ref[mu // 2, :, (mu % 2) * 4 : (mu % 2) * 4 + 4] = g_ref[mu, :, 0:4]

    for h in range(2):
        x = comps(w_ref, h)
        half = slice(h * 8, h * 8 + 8)
        if stage == 0:
            for c in range(18):
                z_out[c, half] = x[c]
            x = [v * 0.25 for v in x]
        elif stage == 1:
            x = [x[c] * (8.0 / 9.0) - z_ref[c, half] * (17.0 / 36.0) for c in range(18)]
            for c in range(18):
                z_out[c, half] = x[c]
        else:
            x = [x[c] * 0.75 - z_ref[c, half] for c in range(18)]
        new = expo_times(x, [s_ref[c, half] for c in range(18)])
        for c in range(18):
            if stage < 2:
                s_out[c, half] = new[c]
            else:
                s_out[h * 2, c] = new[c][0:4]
                s_out[h * 2 + 1, c] = new[c][4:8]

    if stage < 2:
        if stage == 0:
            total = jnp.sum(jnp.where(rows < 4, trace, 0.0))
            mine = where_ref[0] * 4 + where_ref[1]
            act = jnp.where(lane_ids(8) == mine, jnp.broadcast_to(total, (8, NZ)), 0.0)
        else:
            known = ya_ref[8, 6:7] + yb_ref[8, 6:7]
            act = act_ref[...] + jnp.broadcast_to(known, (8, NZ))
        act_out[...] = act
        fill_faces(stage + 1, where_ref, z_out, act, xa_out, xb_out, hop_out)


def fill_faces(stage, where_ref, from_ref, act, xa_out, xb_out, hop_out):
    faces, cuts, _ = message_form(stage)

    def fill(hi_out, lo_out):
        for lo, hi, at in cuts:
            to = slice(at, at + hi - lo)
            for d in range(4):
                hi_out[to, d * 2 : d * 2 + 2] = from_ref[lo:hi, d * 4 + 2 : d * 4 + 4]
                lo_out[to, d * 2 : d * 2 + 2] = from_ref[lo:hi, d * 4 : d * 4 + 2]
        hi_out[faces] = act
        lo_out[faces] = act

    even = is_even(where_ref, 0)
    pl.when(even)(lambda: fill(xa_out, xb_out))
    pl.when(jnp.logical_not(even))(lambda: fill(xb_out, xa_out))
    for lo, hi, at in cuts:
        hop_out[at : at + hi - lo] = from_ref[lo:hi]


def first_kernel(where_ref, l_ref, s_out, xa_out, xb_out, hop_out):
    for d in range(4):
        s_out[:, d * 4 : d * 4 + 4] = l_ref[d]
    fill_faces(0, where_ref, s_out, jnp.zeros((8, NZ), jnp.float32), xa_out, xb_out, hop_out)


def pack_kernel(stage, where_ref, s_ref, xa_ref, xb_ref, ta_ref, tb_ref, act_ref, *rest):
    rest = list(rest)
    before = [rest.pop(0) for _ in range(4)] if stage else [None] * 4
    ya_out, yb_out, qa_out, qb_out, act_out, xp_ref, xm_ref, tp_ref, tm_ref = rest[:9]
    xp_raw, xm_raw, tp_raw, tm_raw = rest[9:]
    even_x, even_y, even_t = (is_even(where_ref, k) for k in range(3))
    faces, cuts, corners = message_form(stage)
    sort_pair(even_x, xa_ref, xb_ref, xp_raw, xm_raw)
    sort_pair(even_t, ta_ref, tb_ref, tp_raw, tm_raw)
    for k, (raw, full) in enumerate(((xp_raw, xp_ref), (xm_raw, xm_ref), (tp_raw, tp_ref), (tm_raw, tm_ref))):
        unpack_faces(stage, raw, before[k], full)

    act = act_ref[...]
    from_plus, from_minus = xp_raw[faces], xm_raw[faces]
    if stage == 1:
        act = act + from_plus + from_minus
    elif stage == 2:
        gx = lane_ids(8) // 4
        plus = gx == (where_ref[0] + 2) % 8
        minus = gx == (where_ref[0] + 6) % 8
        act = act + jnp.where(plus, from_plus, 0.0) + jnp.where(minus, from_minus, 0.0)
    act_out[...] = act

    hi_corner = ((xp_ref, 3), (tp_ref, 5), (tp_ref, 7))
    lo_corner = ((xm_ref, 0), (tm_ref, 8), (tm_ref, 10))

    def fill_y(hi_out, lo_out):
        for d in range(4):
            for x in range(2):
                k = d * 2 + x
                r = d * 4 + x * 2
                for lo, hi, at in cuts:
                    hi_out[at : at + hi - lo, k : k + 1] = s_ref[lo:hi, r + 1 : r + 2]
                    lo_out[at : at + hi - lo, k : k + 1] = s_ref[lo:hi, r : r + 1]
        for out, corner in ((hi_out, hi_corner), (lo_out, lo_corner)):
            for m, c in enumerate(corners):
                for k, (ref, at) in enumerate(corner):
                    row = (m % 2) * 3 + k
                    out[faces + m // 2, row : row + 1] = ref[c, at : at + 1]
            out[faces, 6:7] = act[0:1]

    pl.when(even_y)(lambda: fill_y(ya_out, yb_out))
    pl.when(jnp.logical_not(even_y))(lambda: fill_y(yb_out, ya_out))

    hi = xp_ref[:, T * 2 : T * 2 + 2]
    lo = xm_ref[:, X * 2 : X * 2 + 2]
    mask_t = jnp.broadcast_to(even_t, (18, 2, NZ))
    qa_out[...] = jnp.where(mask_t, hi, lo)
    qb_out[...] = jnp.where(mask_t, lo, hi)


VM = pl.BlockSpec(memory_space=pltpu.VMEM)
SM = pl.BlockSpec(memory_space=pltpu.SMEM)


def arr(*shape):
    return jax.ShapeDtypeStruct(shape, jnp.float32)


def x_message(stage):
    return arr(message_form(stage)[0] + 1, 8, NZ)


def t_message(stage):
    return arr(message_form(stage)[0], 16, NZ)


def call(kernel, outs, scratch, where, *args):
    return pl.pallas_call(
        kernel,
        out_shape=outs,
        in_specs=[SM] + [VM] * len(args),
        out_specs=[VM] * len(outs),
        scratch_shapes=[pltpu.VMEM((*s, NZ), jnp.float32) for s in scratch],
        interpret=INTERPRET,
        compiler_params=pltpu.CompilerParams(vmem_limit_bytes=16 * 2**20),
    )(where, *args)


def run_stage(stage, *args):
    outs = [arr(18, 16, NZ)] if stage < 2 else [arr(4, 18, 4, NZ)]
    if stage < 2:
        outs += [x_message(stage + 1), x_message(stage + 1), t_message(stage + 1)]
        outs += [arr(18, 16, NZ), arr(8, NZ), arr(18, 8, NZ), arr(18, 8, NZ)]
    scratch = [(4, 4, 18, 8), (4, 4, 18, 8), (4, 4, 18, 8), (4, 18, 8), (4, 18, 8), (2, 18, 8), (4, 18, 8)]
    scratch += [(18, 16), (18, 16), (18, 2), (18, 2)] + [message_shape(stage)[:2]] * 2 + [(18, 8), (18, 8)]
    return call(functools.partial(stage_kernel, stage), outs, scratch, *args)


def run_pack(stage, *args):
    outs = [arr(*message_shape(stage))] * 2 + [arr(18, 2, NZ)] * 2 + [arr(8, NZ)]
    outs += [arr(18, 8, NZ)] * 2 + [arr(18, 16, NZ)] * 2
    faces = message_form(stage)[0]
    scratch = [(faces + 1, 8)] * 2 + [(faces, 16)] * 2
    return call(functools.partial(pack_kernel, stage), outs, scratch, *args)


def run_first(where, links):
    outs = [arr(18, 16, NZ), x_message(0), x_message(0), t_message(0)]
    return call(first_kernel, outs, [], where, links)


def swap(value, axis, odd):
    n = lax.axis_size(axis)
    return lax.ppermute(value, axis, [(i, (((i + odd) ^ 1) - odd) % n) for i in range(n)])


def steps(links):
    where = jnp.stack([lax.axis_index(a) for a in ("gx", "gy", "ta")]).astype(jnp.int32)
    state, xa, xb, hop = run_first(where, links.reshape(4, 18, 4, NZ))
    act = jnp.zeros((8, NZ), jnp.float32)
    kept = None
    for k in range(3):
        xb = swap(xb, "gx", 1)
        xa = swap(xa, "gx", 0)
        tb = swap(hop, "ta", 1)
        ta = swap(hop, "ta", 0)
        packed = run_pack(k, where, kept if k else state, xa, xb, ta, tb, act, *(sides if k else ()))
        ya, yb, qa, qb, act, *sides = packed
        yb = swap(yb, "gy", 1)
        qb = swap(qb, "ta", 1)
        qa = swap(qa, "ta", 0)
        ya = swap(ya, "gy", 0)
        halo = (*sides, ya, yb, qa, qb)
        if k == 0:
            state, xa, xb, hop, kept, act, *before = run_stage(0, where, state, *halo)
        elif k == 1:
            state, xa, xb, hop, kept, act, *before = run_stage(1, where, state, *halo, kept, *before, act)
        else:
            lane = jnp.arange(NZ)
            far_y = lane % 4 == (where[1] + 2) % 4
            act = act[0] + jnp.where(far_y, ya[8, 6], 0.0)
            other = lax.ppermute(act, "gx", [(i, (i + 4) % 8) for i in range(8)])
            state = run_stage(2, where, state, *halo, kept, *before)[0]
            near_x = (lane // 4 - where[0] + 2) % 8 < 5
            act = jnp.where(near_x, act, other)
    flowed = state.reshape(links.shape)
    sites_slice = 6.0 * links.shape[4] * lax.axis_size("gx") * links.shape[5] * lax.axis_size("gy") * links.shape[7]
    return (flowed, (jnp.sum(act[:32]) / sites_slice).reshape(1))


def solution(mesh):
    spec = P(None, None, None, None, "gx", "gy", "ta", None)
    return jax.shard_map(steps, mesh=mesh, in_specs=(spec,), out_specs=(spec, P("ta")), check_vma=False)
```
